256 devices in a mesh: lat: 128 (over z, x, y), fld: 2 (over core).
Axes of the slice: x: 4, y: 4, z: 8, core: 2. Of those that a mesh axis runs over, the one named last changes fastest.
Arguments:
- grid_fields: bfloat16 [3, 16, 256, 2, 1152], P(None, 'fld', 'lat'), may hold values from -6 to 6
- legendre_basis: bfloat16 [640, 2, 256, 640], P('lat', 'fld'), may hold values from -0.25 to 0.25
- owner_list: int32 [640], replicated, may hold values from 0 to 639, as said below
- wave_speed: float32 [16], P('fld'), may hold values from 1e-06 to 0.01
Outputs:
- balanced_spectra: bfloat16 [640, 2, 3, 16, 640], P('lat', None, None, 'fld')
- balanced_grid: bfloat16 [3, 16, 256, 2, 1152], P(None, 'fld', 'lat')
The draws below stay inside these ranges and needn't reach their ends.
Inputs may be any that keep to these rules, and one draw needn't show every extreme that they name: owner_list is a permutation of the 640 wavenumbers; slot d * 5 + r holds a wavenumber of r * 128 to r * 128 + 127, and for each index d of lat the slots of rounds 2 i and 2 i + 1 hold wavenumbers that add up to (4 i + 2) * 128 - 1.
All inputs are finite; a program needn't handle non-finite values.
Results may differ from the reference program's by a relative error of at most 0.0074.
Values may be sent and summed in bfloat16 or wider, within the bound.
No kernel may reach another device: no remote copies, remote signals or barrier semaphores. Data moves between devices by JAX's collectives and lax.ppermute only.
A program may use at most 128 MiB of HBM per device.

```python
import math
import jax
import jax.numpy as jnp
from jax import lax

NM = 640
MODES = 16
HALF = 256
PPAD = 1152
N_LAT = 128


def draw_owner_list(key, part):
    rounds = NM // N_LAT
    pieces = []
    for round_index in range(rounds):
        shuffled = jax.random.permutation(jax.random.fold_in(key, 17 + round_index // 2), N_LAT).astype(jnp.int32)
        if round_index % 2 == 0:
            placed = shuffled
        else:
            placed = N_LAT - 1 - shuffled
        pieces.append(round_index * N_LAT + placed)
    return jnp.stack(pieces, axis=1).reshape(-1).astype(jnp.int32)


def block_levels(key, shape, shards, least, top_value):
    def one(position, parts):
        heights = jax.random.uniform(jax.random.fold_in(jax.random.fold_in(key, 6), position), (parts,), jnp.float32, least / len(shards), top_value / len(shards))
        return jnp.repeat(jnp.exp(heights), shape[position] // parts).reshape((-1,) + (1,) * (len(shape) - position - 1))

    loudness = one(*shards[0])
    for cut in shards[1:]:
        loudness = loudness * one(*cut)
    return loudness


def gaussian(key, dims, scale, limit, split=(), kind=jnp.bfloat16):
    level = block_levels(key, dims, split, -0.22, 0.18) if split else 1.0
    values = jax.random.normal(key, dims, jnp.float32) * scale * level
    return jnp.minimum(jnp.maximum(values, -limit), limit).astype(kind)


def setup_inputs(seed: int = 0) -> dict:
    streams_of = jax.random.split(jax.random.key(seed), 5)
    grid_fields = gaussian(streams_of[0], (3, MODES, HALF, 2, PPAD), 1.0, 6.0, ((1, 2), (2, 128)))
    legendre_basis = gaussian(streams_of[1], (NM, 2, HALF, NM), (2 * HALF) ** -0.5, 0.25, ((0, 128), (1, 2)))
    owner_list = draw_owner_list(jax.random.fold_in(streams_of[4], 71), 0)
    wave_speed = jnp.clip(jnp.exp(math.log(0.01) - 9.2103404 * jax.random.uniform(streams_of[3], (MODES,), jnp.float32) ** block_levels(streams_of[3], (MODES,), ((0, 2),), -0.2, 0.2)), 9.999999974752427e-07, 0.01)
    return {"grid_fields": grid_fields, "legendre_basis": legendre_basis, "owner_list": owner_list, "wave_speed": wave_speed}


def row_table(pair_index, waves, padded, wave_count):
    points = 20 + 4 * pair_index
    highest = jnp.minimum(wave_count - 1, (points - 1) // 2)
    column = jnp.arange(padded, dtype=jnp.int32)
    phase_steps = column[:, None] * waves[None, :] % points
    angles = phase_steps.astype(jnp.float32) * (jnp.float32(2.0 * math.pi) / points.astype(jnp.float32))
    scaling = 1.0 / jnp.sqrt(points.astype(jnp.float32))
    inside = (column[:, None] < points) & (waves[None, :] <= highest)
    cosine = jnp.where(inside, jnp.cos(angles) * scaling, 0.0)
    sine_part = jnp.where(inside, -jnp.sin(angles) * scaling, 0.0)
    return jnp.stack([cosine, sine_part], axis=1).astype(jnp.bfloat16)

def balance(spectra, speeds, waves):
    totals = jnp.arange(spectra.shape[-1], dtype=jnp.int32)
    degree = totals.astype(jnp.float32)
    laplace = degree * (degree + 1.0)
    stiffness = laplace[None, :] * speeds[:, None]
    retained = 1.0 / (1.0 + stiffness)
    root_term = jnp.sqrt(stiffness)
    removed = stiffness * retained
    vorticity = spectra[:, :, 0]
    divergence = spectra[:, :, 1]
    geopotential = spectra[:, :, 2]
    rossby_part = (root_term * vorticity - geopotential) * retained
    result = jnp.stack([retained * vorticity + removed * root_term * rossby_part, retained * divergence, retained * geopotential - removed * rossby_part], axis=2)
    triangle = totals[None, :] >= waves[:, None]
    return jnp.where(triangle[:, None, None, None, :], result, 0.0)

def reference(grid_fields, legendre_basis, owner_list, wave_speed):
    padded = grid_fields.shape[4]
    wave_count = owner_list.shape[0]
    half_count = grid_fields.shape[2]
    pair_ids = jnp.arange(half_count, dtype=jnp.int32)

    def analyse_row(inputs):
        pair_index, row_values = inputs
        tables = row_table(pair_index, owner_list, padded, wave_count).astype(jnp.float32)
        return jnp.einsum('fkhj,jts->tfkhs', row_values.astype(jnp.float32), tables).astype(jnp.bfloat16)
    fourier = lax.map(analyse_row, (pair_ids, jnp.moveaxis(grid_fields, 2, 0)))
    by_slot = jnp.moveaxis(fourier, 5, 0)

    def legendre(inputs):
        row_values, tables = inputs
        return jnp.einsum('ptfkh,hpn->tfkn', row_values.astype(jnp.float32), tables.astype(jnp.float32))
    spectra = lax.map(legendre, (by_slot, legendre_basis))
    balanced = balance(spectra, wave_speed, owner_list).astype(jnp.bfloat16)

    def synthesise(inputs):
        tables, values = inputs
        return jnp.einsum('hpn,tfkn->ptfkh', tables.astype(jnp.float32), values.astype(jnp.float32)).astype(jnp.bfloat16)
    fourier_new = lax.map(synthesise, (legendre_basis, balanced))
    weights = jnp.where(owner_list == 0, 1.0, 2.0).astype(jnp.float32)

    def compose_row(inputs):
        pair_index, values = inputs
        tables = row_table(pair_index, owner_list, padded, wave_count).astype(jnp.float32)
        scaled = values.astype(jnp.float32) * weights[:, None, None, None, None]
        return jnp.einsum('stfkh,jts->fkhj', scaled, tables).astype(jnp.bfloat16)
    grid_new = lax.map(compose_row, (pair_ids, jnp.moveaxis(fourier_new, 1, 0)))
    return (balanced, jnp.moveaxis(grid_new, 0, 2))
```

```python
import math

import jax
import jax.numpy as jnp
from jax import lax
from jax.experimental import pallas as pl
from jax.experimental.pallas import tpu as pltpu
from jax.sharding import PartitionSpec as P

F32 = jnp.float32
BF16 = jnp.bfloat16
LANES = 128
SINE_TERMS = (-1.0 / 6.0, 1.0 / 120.0, -1.0 / 5040.0, 1.0 / 362880.0)
COSINE_TERMS = (-1.0 / 2.0, 1.0 / 24.0, -1.0 / 720.0, 1.0 / 40320.0, -1.0 / 3628800.0)


def cosine_sine(product, quarters, quarter, turn):
    steps = jnp.floor(product * quarters + 0.5)
    angle = (product - steps * quarter) * turn
    square = angle * angle
    sine = F32(SINE_TERMS[-1])
    for term in SINE_TERMS[-2::-1]:
        sine = sine * square + F32(term)
    sine = angle + angle * square * sine
    cosine = F32(COSINE_TERMS[-1])
    for term in COSINE_TERMS[-2::-1]:
        cosine = cosine * square + F32(term)
    cosine = 1.0 + square * cosine
    quadrant = steps - 4.0 * jnp.floor(steps * 0.25)
    odd = (quadrant == 1.0) | (quadrant == 3.0)
    first = jnp.where(odd, sine, cosine)
    second = jnp.where(odd, cosine, sine)
    first = jnp.where((quadrant == 1.0) | (quadrant == 2.0), -first, first)
    second = jnp.where(quadrant >= 2.0, -second, second)
    return first, second


def analyse_kernel(position_ref, waves_ref, rows_ref, table_ref, out_ref, stage_ref):
    pair_count, lines, padded = rows_ref.shape
    half_lines = lines // 2
    rounds = table_ref.shape[1] // (2 * LANES)
    wave_count = rounds * LANES
    chunk = 32

    def build(step, carry):
        pair = step // rounds
        turn_round = step % rounds
        points = 20 + 4 * (position_ref[0] * pair_count + pair)
        highest = jnp.minimum(wave_count - 1, (points - 1) // 2).astype(F32)
        points_row = jnp.full((1, LANES), points.astype(F32), F32)
        quarters = 4.0 / points_row
        quarter = points_row * 0.25
        turn = F32(2.0 * math.pi) / points_row
        scaling = 1.0 / jnp.sqrt(points_row)
        waves_row = waves_ref[pl.ds(turn_round, 1), :]
        waves = jnp.transpose(jnp.broadcast_to(waves_row, (LANES, LANES)))
        for first in range(0, LANES, chunk):
            wave = waves[first : first + chunk]
            column = lax.broadcasted_iota(jnp.int32, (chunk, LANES), 1).astype(F32)
            cosine, sine = cosine_sine(wave * column, quarters, quarter, turn)
            shift_cosine, shift_sine = cosine_sine(wave * F32(LANES), quarters, quarter, turn)
            amplitude = jnp.where(wave <= highest, scaling, 0.0)
            real = cosine * amplitude
            imaginary = -sine * amplitude
            for block in range(padded // LANES):
                place = pl.ds(block * LANES, LANES)
                table_ref[pair, pl.ds(turn_round * LANES + first, chunk), place] = real.astype(BF16)
                table_ref[pair, pl.ds(wave_count + turn_round * LANES + first, chunk), place] = (
                    imaginary.astype(BF16)
                )
                if block + 1 < padded // LANES:
                    real, imaginary = (
                        real * shift_cosine + imaginary * shift_sine,
                        imaginary * shift_cosine - real * shift_sine,
                    )
        return carry

    lax.fori_loop(0, pair_count * rounds, build, 0)
    column = lax.broadcasted_iota(jnp.int32, (lines, padded), 1)
    spare = jnp.zeros((LANES - rounds * half_lines, LANES), F32)
    for pair in range(pair_count):
        points = 20 + 4 * (position_ref[0] * pair_count + pair)
        rows = jnp.where(column < points, rows_ref[pair].astype(F32), 0.0).astype(BF16)
        fourier = lax.dot_general(
            rows, table_ref[pair], (((1,), (1,)), ((), ())), preferred_element_type=F32
        )
        for part in range(2):
            for hemi in range(2):
                pieces = [
                    fourier[
                        hemi * half_lines : (hemi + 1) * half_lines,
                        part * wave_count + r * LANES : part * wave_count + (r + 1) * LANES,
                    ]
                    for r in range(rounds)
                ]
                packed = jnp.transpose(jnp.concatenate(pieces + [spare], axis=0))
                stage_ref[pl.ds(part * 4 + hemi * 2 + pair, LANES, stride=8), :] = packed
    out_ref[...] = stage_ref[...].astype(BF16)


def balance_kernel(
    hemi_ref, own_wave_ref, speeds_ref, got_ref, basis_ref, other_ref,
    balanced_ref, out_ref, stage_ref, line_ref, wide_ref,
):
    slot_count, half_count, totals_count = basis_ref.shape
    lines = balanced_ref.shape[0] // slot_count
    half_lines = lines // 2
    modes = speeds_ref.shape[0]
    hemi_own = hemi_ref[0]
    hemi_other = 1 - hemi_own
    stage_ref[...] = got_ref[...].astype(F32)
    for group in range(4):
        for pair in range(2):
            line_ref[group, pl.ds(pair, LANES, stride=2), :] = stage_ref[
                pl.ds(group * 2 + pair, LANES, stride=8), :
            ]
    own_rows = [jnp.transpose(line_ref[2 * part + hemi_own]) for part in range(2)]
    other_rows = [jnp.transpose(line_ref[2 * part + hemi_other]) for part in range(2)]

    totals = lax.broadcasted_iota(jnp.int32, (modes, totals_count), 1)
    degree = totals.astype(F32)
    stiffness = degree * (degree + 1.0) * speeds_ref[...]
    retained = 1.0 / (1.0 + stiffness)
    root_term = jnp.sqrt(stiffness)
    removed = stiffness * retained

    for r in range(slot_count):
        span = slice(r * half_lines, (r + 1) * half_lines)
        own = jnp.concatenate([own_rows[0][span], own_rows[1][span]], axis=0).astype(BF16)
        other = jnp.concatenate([other_rows[0][span], other_rows[1][span]], axis=0).astype(BF16)
        spectra = jnp.dot(own, basis_ref[r], preferred_element_type=F32) + jnp.dot(
            other, other_ref[r], preferred_element_type=F32
        )
        inside = totals >= own_wave_ref[r]
        pieces = []
        for part in range(2):
            base = part * half_lines
            vorticity = spectra[base : base + modes]
            divergence = spectra[base + modes : base + 2 * modes]
            geopotential = spectra[base + 2 * modes : base + 3 * modes]
            rossby_part = (root_term * vorticity - geopotential) * retained
            pieces.append(jnp.where(inside, retained * vorticity + removed * root_term * rossby_part, 0.0))
            pieces.append(jnp.where(inside, retained * divergence, 0.0))
            pieces.append(jnp.where(inside, retained * geopotential - removed * rossby_part, 0.0))
        result = jnp.concatenate(pieces, axis=0).astype(BF16)
        balanced_ref[r * lines : (r + 1) * lines, :] = result
        weight = jnp.where(own_wave_ref[r] == 0, 1.0, 2.0).astype(F32)
        scaled = result.astype(F32) * weight
        wide_ref[pl.ds(r * half_lines, half_lines), :] = scaled[:half_lines]
        wide_ref[pl.ds(LANES + r * half_lines, half_lines), :] = scaled[half_lines:]
    spare = LANES - slot_count * half_lines
    for part in range(2):
        wide_ref[pl.ds((part + 1) * LANES - spare, spare), :] = jnp.zeros((spare, totals_count), F32)

    tall = jnp.transpose(wide_ref[...])
    lane = lax.broadcasted_iota(jnp.int32, tall.shape, 1) % LANES
    own_sum = jnp.zeros((half_count, 2 * LANES), F32)
    other_sum = jnp.zeros((half_count, 2 * LANES), F32)
    for r in range(slot_count):
        chosen = (lane >= r * half_lines) & (lane < (r + 1) * half_lines)
        values = jnp.where(chosen, tall, 0.0).astype(BF16)
        own_sum += jnp.dot(basis_ref[r], values, preferred_element_type=F32)
        other_sum += jnp.dot(other_ref[r], values, preferred_element_type=F32)
    for part in range(2):
        line_ref[2 * part + hemi_own] = own_sum[:, part * LANES : (part + 1) * LANES]
        line_ref[2 * part + hemi_other] = other_sum[:, part * LANES : (part + 1) * LANES]
    for group in range(4):
        for pair in range(2):
            stage_ref[pl.ds(group * 2 + pair, LANES, stride=8), :] = line_ref[
                group, pl.ds(pair, LANES, stride=2), :
            ]
    out_ref[...] = stage_ref[...].astype(BF16)


def compose_kernel(position_ref, got_ref, table_ref, out_ref, stage_ref):
    pair_count, lines, padded = out_ref.shape
    half_lines = lines // 2
    rounds = table_ref.shape[1] // (2 * LANES)
    stage_ref[...] = got_ref[...].astype(F32)
    column = lax.broadcasted_iota(jnp.int32, (lines, padded), 1)
    for pair in range(pair_count):
        halves = []
        for hemi in range(2):
            pieces = []
            for part in range(2):
                slab = jnp.transpose(stage_ref[pl.ds(part * 4 + hemi * 2 + pair, LANES, stride=8), :])
                pieces += [slab[r * half_lines : (r + 1) * half_lines] for r in range(rounds)]
            halves.append(jnp.concatenate(pieces, axis=1))
        values = jnp.concatenate(halves, axis=0).astype(BF16)
        grid = jnp.dot(values, table_ref[pair], preferred_element_type=F32)
        points = 20 + 4 * (position_ref[0] * pair_count + pair)
        out_ref[pair] = jnp.where(column < points, grid, 0.0).astype(BF16)


def smem():
    return pl.BlockSpec(memory_space=pltpu.SMEM)


def vmem():
    return pl.BlockSpec(memory_space=pltpu.VMEM)


def per_device(grid_fields, legendre_basis, owner_list, wave_speed):
    field_count, mode_count, pair_count, hemis, padded = grid_fields.shape
    slot_count, _, half_count, totals_count = legendre_basis.shape
    wave_count = owner_list.shape[0]
    peers = wave_count // slot_count
    lines = field_count * mode_count * hemis
    position = lax.axis_index("lat").astype(jnp.int32)
    hemi = lax.axis_index("fld").astype(jnp.int32)
    position_one = position.reshape(1)
    basis = legendre_basis.reshape(slot_count, half_count, totals_count)
    other = lax.ppermute(basis, "fld", [(0, 1), (1, 0)])
    own_wave = lax.dynamic_slice_in_dim(owner_list, position * slot_count, slot_count)
    waves = jnp.pad(
        jnp.transpose(owner_list.reshape(peers, slot_count)).astype(F32), ((0, 8 - slot_count), (0, 0))
    )
    rows = jnp.transpose(grid_fields, (2, 3, 0, 1, 4)).reshape(pair_count, lines, padded)
    params = pltpu.CompilerParams(vmem_limit_bytes=48 << 20)
    exchange = jax.ShapeDtypeStruct((peers * 8, LANES), BF16)

    table, sent = pl.pallas_call(
        analyse_kernel,
        out_shape=(jax.ShapeDtypeStruct((pair_count, 2 * wave_count, padded), BF16), exchange),
        in_specs=[smem(), vmem(), vmem()],
        out_specs=(vmem(), vmem()),
        scratch_shapes=[pltpu.VMEM((peers * 8, LANES), F32)],
        compiler_params=params,
        name="row_analysis",
    )(position_one, waves, rows)
    got = lax.all_to_all(sent.reshape(peers, 8, LANES), "lat", 0, 0, tiled=True)
    balanced, returned = pl.pallas_call(
        balance_kernel,
        out_shape=(jax.ShapeDtypeStruct((slot_count * lines, totals_count), BF16), exchange),
        in_specs=[smem(), smem(), vmem(), vmem(), vmem(), vmem()],
        out_specs=(vmem(), vmem()),
        scratch_shapes=[
            pltpu.VMEM((peers * 8, LANES), F32),
            pltpu.VMEM((4, half_count, LANES), F32),
            pltpu.VMEM((2 * LANES, totals_count), F32),
        ],
        compiler_params=params,
        name="legendre_balance",
    )(hemi.reshape(1), own_wave, wave_speed.reshape(mode_count, 1), got.reshape(peers * 8, LANES), basis, other)
    back = lax.all_to_all(returned.reshape(peers, 8, LANES), "lat", 0, 0, tiled=True)
    grid = pl.pallas_call(
        compose_kernel,
        out_shape=jax.ShapeDtypeStruct((pair_count, lines, padded), BF16),
        in_specs=[smem(), vmem(), vmem()],
        out_specs=vmem(),
        scratch_shapes=[pltpu.VMEM((peers * 8, LANES), F32)],
        compiler_params=params,
        name="row_synthesis",
    )(position_one, back.reshape(peers * 8, LANES), table)
    balanced_grid = jnp.transpose(
        grid.reshape(pair_count, hemis, field_count, mode_count, padded), (2, 3, 0, 1, 4)
    )
    balanced_spectra = balanced.reshape(slot_count, 2, field_count, mode_count, totals_count)
    return (balanced_spectra, balanced_grid)


def solution(mesh):
    placed = (P(None, "fld", "lat", None, None), P("lat", "fld", None, None), P(), P("fld"))
    return jax.shard_map(
        per_device,
        mesh=mesh,
        in_specs=placed,
        out_specs=(P("lat", None, None, "fld", None), P(None, "fld", "lat", None, None)),
        check_vma=False,
    )
```

```python
import math

import jax
import jax.numpy as jnp
from jax import lax
from jax.experimental import pallas as pl
from jax.experimental.pallas import tpu as pltpu
from jax.sharding import PartitionSpec as P

F32 = jnp.float32
BF16 = jnp.bfloat16
LANES = 128
SINE_TERMS = (-1.0 / 6.0, 1.0 / 120.0, -1.0 / 5040.0, 1.0 / 362880.0)
COSINE_TERMS = (-1.0 / 2.0, 1.0 / 24.0, -1.0 / 720.0, 1.0 / 40320.0, -1.0 / 3628800.0)


def cosine_sine(product, quarters, quarter, turn):
    steps = jnp.floor(product * quarters + 0.5)
    angle = (product - steps * quarter) * turn
    square = angle * angle
    sine = F32(SINE_TERMS[-1])
    for term in SINE_TERMS[-2::-1]:
        sine = sine * square + F32(term)
    sine = angle + angle * square * sine
    cosine = F32(COSINE_TERMS[-1])
    for term in COSINE_TERMS[-2::-1]:
        cosine = cosine * square + F32(term)
    cosine = 1.0 + square * cosine
    quadrant = steps - 4.0 * jnp.floor(steps * 0.25)
    odd = (quadrant == 1.0) | (quadrant == 3.0)
    first = jnp.where(odd, sine, cosine)
    second = jnp.where(odd, cosine, sine)
    first = jnp.where((quadrant == 1.0) | (quadrant == 2.0), -first, first)
    second = jnp.where(quadrant >= 2.0, -second, second)
    return first, second


def mirror_blocks(values):
    row = lax.broadcasted_iota(jnp.int32, (LANES, LANES), 0)
    column = lax.broadcasted_iota(jnp.int32, (LANES, LANES), 1)
    flip = jnp.where(row + column == LANES - 1, 1.0, 0.0).astype(BF16)
    blocks = values.shape[1] // LANES
    pieces = [
        jnp.dot(values[:, k * LANES : (k + 1) * LANES], flip, preferred_element_type=F32)
        for k in reversed(range(blocks))
    ]
    return jnp.concatenate(pieces, axis=1)


def row_constants(points):
    points_row = jnp.full((1, LANES), points.astype(F32), F32)
    return 4.0 / points_row, points_row * 0.25, F32(2.0 * math.pi) / points_row, 1.0 / jnp.sqrt(points_row)


def analyse_kernel(position_ref, waves_ref, rows_ref, table_ref, out_ref, stage_ref, wave_ref):
    pair_count, lines, padded = rows_ref.shape
    half_lines = lines // 2
    rounds = waves_ref.shape[0]
    wave_count = rounds * LANES
    width = table_ref.shape[2]
    chunk = 32
    all_points = [20 + 4 * (position_ref[0] * pair_count + pair) for pair in range(pair_count)]

    flat = jnp.concatenate([waves_ref[...].astype(F32), jnp.zeros((8 - rounds, LANES), F32)], axis=0)
    quantities = [flat]
    for points in all_points:
        quarters, quarter, turn, _ = row_constants(points)
        quantities += cosine_sine(flat * F32(LANES), quarters, quarter, turn)
    filler = jnp.zeros((LANES - 8 * len(quantities), LANES), F32)
    columns = jnp.transpose(jnp.concatenate(quantities + [filler], axis=0))
    for r in range(rounds):
        wave_ref[r * LANES : (r + 1) * LANES, :] = columns if r == 0 else pltpu.roll(columns, LANES - r, 1)

    column = lax.broadcasted_iota(jnp.int32, (chunk, LANES), 1).astype(F32)
    for r in range(rounds):
        mine = wave_ref[pl.ds(r, LANES, stride=rounds), :]
        for first in range(0, LANES, chunk):
            part = mine[first : first + chunk]
            wave = jnp.broadcast_to(part[:, 0:1], (chunk, LANES))
            for pair in range(pair_count):
                points = all_points[pair]
                quarters, quarter, turn, scaling = row_constants(points)
                highest = jnp.minimum(wave_count - 1, (points - 1) // 2).astype(F32)
                spot = 8 + 16 * pair
                shift_cosine = jnp.broadcast_to(part[:, spot : spot + 1], (chunk, LANES))
                shift_sine = jnp.broadcast_to(part[:, spot + 8 : spot + 9], (chunk, LANES))
                cosine, sine = cosine_sine(wave * column, quarters, quarter, turn)
                amplitude = jnp.where(wave <= highest, scaling, 0.0)
                real = cosine * amplitude
                imaginary = -sine * amplitude
                top = r * LANES + first
                for block in range(width // LANES):
                    place = slice(block * LANES, (block + 1) * LANES)
                    table_ref[pair, top : top + chunk, place] = real.astype(BF16)
                    table_ref[pair, wave_count + top : wave_count + top + chunk, place] = imaginary.astype(BF16)
                    if block + 1 < width // LANES:
                        real, imaginary = (
                            real * shift_cosine + imaginary * shift_sine,
                            imaginary * shift_cosine - real * shift_sine,
                        )

    place = lax.broadcasted_iota(jnp.int32, (lines, width), 1)
    spare = jnp.zeros((LANES - rounds * half_lines, LANES), F32)
    for pair in range(pair_count):
        points = all_points[pair]
        middle = points // 2
        mirrored = pltpu.roll(mirror_blocks(rows_ref[pair]), points + 1, 1)[:, :width]
        rows = rows_ref[pair, :, :width].astype(F32)
        between = (place >= 1) & (place < middle)
        even = rows + jnp.where(between, mirrored, 0.0)
        even = jnp.where(place <= middle, even, 0.0).astype(BF16)
        odd = jnp.where(between, rows - mirrored, 0.0).astype(BF16)
        for part, folded in enumerate((even, odd)):
            fourier = lax.dot_general(
                folded,
                table_ref[pair, part * wave_count : (part + 1) * wave_count, :],
                (((1,), (1,)), ((), ())),
                preferred_element_type=F32,
            )
            for hemi in range(2):
                pieces = [
                    fourier[hemi * half_lines : (hemi + 1) * half_lines, r * LANES : (r + 1) * LANES]
                    for r in range(rounds)
                ]
                packed = jnp.transpose(jnp.concatenate(pieces + [spare], axis=0))
                stage_ref[pl.ds(part * 4 + hemi * 2 + pair, LANES, stride=8), :] = packed
    out_ref[...] = stage_ref[...].astype(BF16)


def balance_kernel(
    hemi_ref, own_wave_ref, speeds_ref, got_ref, basis_hbm, other_ref,
    balanced_ref, out_ref, stage_ref, line_ref, wide_ref, basis_ref, arrived,
):
    fetch = pltpu.make_async_copy(basis_hbm, basis_ref, arrived)
    fetch.start()
    slot_count, half_count, totals_count = basis_ref.shape
    lines = balanced_ref.shape[0] // slot_count
    half_lines = lines // 2
    modes = speeds_ref.shape[0]
    hemi_own = hemi_ref[0]
    hemi_other = 1 - hemi_own
    stage_ref[...] = got_ref[...].astype(F32)
    for group in range(4):
        for pair in range(2):
            line_ref[group, pl.ds(pair, LANES, stride=2), :] = stage_ref[
                pl.ds(group * 2 + pair, LANES, stride=8), :
            ]
    own_rows = [jnp.transpose(line_ref[2 * part + hemi_own]) for part in range(2)]
    other_rows = [jnp.transpose(line_ref[2 * part + hemi_other]) for part in range(2)]

    totals = lax.broadcasted_iota(jnp.int32, (modes, totals_count), 1)
    degree = totals.astype(F32)
    stiffness = degree * (degree + 1.0) * speeds_ref[...]
    retained = 1.0 / (1.0 + stiffness)
    root_term = jnp.sqrt(stiffness)
    removed = stiffness * retained

    fetch.wait()
    for r in range(slot_count):
        span = slice(r * half_lines, (r + 1) * half_lines)
        own = jnp.concatenate([own_rows[0][span], own_rows[1][span]], axis=0).astype(BF16)
        other = jnp.concatenate([other_rows[0][span], other_rows[1][span]], axis=0).astype(BF16)
        spectra = jnp.dot(own, basis_ref[r], preferred_element_type=F32) + jnp.dot(
            other, other_ref[r], preferred_element_type=F32
        )
        inside = totals >= own_wave_ref[r]
        pieces = []
        for part in range(2):
            base = part * half_lines
            vorticity = spectra[base : base + modes]
            divergence = spectra[base + modes : base + 2 * modes]
            geopotential = spectra[base + 2 * modes : base + 3 * modes]
            rossby_part = (root_term * vorticity - geopotential) * retained
            pieces.append(jnp.where(inside, retained * vorticity + removed * root_term * rossby_part, 0.0))
            pieces.append(jnp.where(inside, retained * divergence, 0.0))
            pieces.append(jnp.where(inside, retained * geopotential - removed * rossby_part, 0.0))
        result = jnp.concatenate(pieces, axis=0).astype(BF16)
        balanced_ref[r * lines : (r + 1) * lines, :] = result
        weight = jnp.where(own_wave_ref[r] == 0, 1.0, 2.0).astype(F32)
        scaled = result.astype(F32) * weight
        wide_ref[pl.ds(r * half_lines, half_lines), :] = scaled[:half_lines]
        wide_ref[pl.ds(LANES + r * half_lines, half_lines), :] = scaled[half_lines:]
    spare = LANES - slot_count * half_lines
    for part in range(2):
        wide_ref[pl.ds((part + 1) * LANES - spare, spare), :] = jnp.zeros((spare, totals_count), F32)

    tall = jnp.transpose(wide_ref[...])
    lane = lax.broadcasted_iota(jnp.int32, tall.shape, 1) % LANES
    own_sum = jnp.zeros((half_count, 2 * LANES), F32)
    other_sum = jnp.zeros((half_count, 2 * LANES), F32)
    for r in range(slot_count):
        chosen = (lane >= r * half_lines) & (lane < (r + 1) * half_lines)
        values = jnp.where(chosen, tall, 0.0).astype(BF16)
        own_sum += jnp.dot(basis_ref[r], values, preferred_element_type=F32)
        other_sum += jnp.dot(other_ref[r], values, preferred_element_type=F32)
    for part in range(2):
        line_ref[2 * part + hemi_own] = own_sum[:, part * LANES : (part + 1) * LANES]
        line_ref[2 * part + hemi_other] = other_sum[:, part * LANES : (part + 1) * LANES]
    for group in range(4):
        for pair in range(2):
            stage_ref[pl.ds(group * 2 + pair, LANES, stride=8), :] = line_ref[
                group, pl.ds(pair, LANES, stride=2), :
            ]
    out_ref[...] = stage_ref[...].astype(BF16)


def compose_kernel(position_ref, got_ref, table_ref, out_ref, stage_ref):
    pair_count, lines, padded = out_ref.shape
    half_lines = lines // 2
    wave_count = table_ref.shape[1] // 2
    width = table_ref.shape[2]
    rounds = wave_count // LANES
    stage_ref[...] = got_ref[...].astype(F32)
    place = lax.broadcasted_iota(jnp.int32, (lines, padded), 1)
    tail = jnp.zeros((lines, padded - width), F32)
    for pair in range(pair_count):
        waves = []
        for part in range(2):
            halves = []
            for hemi in range(2):
                slab = jnp.transpose(stage_ref[pl.ds(part * 4 + hemi * 2 + pair, LANES, stride=8), :])
                pieces = [slab[r * half_lines : (r + 1) * half_lines] for r in range(rounds)]
                halves.append(jnp.concatenate(pieces, axis=1))
            values = jnp.concatenate(halves, axis=0).astype(BF16)
            waves.append(
                jnp.dot(
                    values,
                    table_ref[pair, part * wave_count : (part + 1) * wave_count, :],
                    preferred_element_type=F32,
                )
            )
        even, odd = waves
        points = 20 + 4 * (position_ref[0] * pair_count + pair)
        turned = mirror_blocks((even - odd).astype(BF16))
        shift = points + padded - width + 1
        shift = jnp.where(shift >= padded, shift - padded, shift)
        far = pltpu.roll(jnp.concatenate([turned, tail], axis=1), shift, 1)
        near = jnp.concatenate([even + odd, tail], axis=1)
        grid = jnp.where(place <= points // 2, near, far)
        out_ref[pair] = jnp.where(place < points, grid, 0.0).astype(BF16)


def smem():
    return pl.BlockSpec(memory_space=pltpu.SMEM)


def vmem():
    return pl.BlockSpec(memory_space=pltpu.VMEM)


def per_device(grid_fields, legendre_basis, owner_list, wave_speed):
    field_count, mode_count, pair_count, hemis, padded = grid_fields.shape
    slot_count, _, half_count, totals_count = legendre_basis.shape
    wave_count = owner_list.shape[0]
    peers = wave_count // slot_count
    lines = field_count * mode_count * hemis
    position = lax.axis_index("lat").astype(jnp.int32)
    hemi = lax.axis_index("fld").astype(jnp.int32)
    position_one = position.reshape(1)
    basis = legendre_basis.reshape(slot_count, half_count, totals_count)
    other = lax.ppermute(basis, "fld", [(0, 1), (1, 0)])
    own_wave = lax.dynamic_slice_in_dim(owner_list, position * slot_count, slot_count)
    waves = owner_list.reshape(slot_count, peers)
    width = (padded // 2 + LANES - 1) // LANES * LANES
    rows = jnp.transpose(grid_fields, (2, 3, 0, 1, 4)).reshape(pair_count, lines, padded)
    params = pltpu.CompilerParams(vmem_limit_bytes=24 << 20)
    exchange = jax.ShapeDtypeStruct((peers * 8, LANES), BF16)

    table, sent = pl.pallas_call(
        analyse_kernel,
        out_shape=(jax.ShapeDtypeStruct((pair_count, 2 * wave_count, width), BF16), exchange),
        in_specs=[smem(), vmem(), vmem()],
        out_specs=(vmem(), vmem()),
        scratch_shapes=[pltpu.VMEM((peers * 8, LANES), F32), pltpu.VMEM((wave_count, LANES), F32)],
        compiler_params=params,
        name="row_analysis",
    )(position_one, waves, rows)
    got = lax.all_to_all(sent.reshape(peers, 8, LANES), "lat", 0, 0, tiled=True)
    balanced, returned = pl.pallas_call(
        balance_kernel,
        out_shape=(jax.ShapeDtypeStruct((slot_count * lines, totals_count), BF16), exchange),
        in_specs=[smem(), smem(), vmem(), vmem(), pl.BlockSpec(memory_space=pltpu.MemorySpace.HBM), vmem()],
        out_specs=(vmem(), vmem()),
        scratch_shapes=[
            pltpu.VMEM((peers * 8, LANES), F32),
            pltpu.VMEM((4, half_count, LANES), F32),
            pltpu.VMEM((2 * LANES, totals_count), F32),
            pltpu.VMEM((slot_count, half_count, totals_count), BF16),
            pltpu.SemaphoreType.DMA,
        ],
        compiler_params=params,
        name="legendre_balance",
    )(hemi.reshape(1), own_wave, wave_speed.reshape(mode_count, 1), got.reshape(peers * 8, LANES), basis, other)
    back = lax.all_to_all(returned.reshape(peers, 8, LANES), "lat", 0, 0, tiled=True)
    grid = pl.pallas_call(
        compose_kernel,
        out_shape=jax.ShapeDtypeStruct((pair_count, lines, padded), BF16),
        in_specs=[smem(), vmem(), vmem()],
        out_specs=vmem(),
        scratch_shapes=[pltpu.VMEM((peers * 8, LANES), F32)],
        compiler_params=params,
        name="row_synthesis",
    )(position_one, back.reshape(peers * 8, LANES), table)
    balanced_grid = jnp.transpose(
        grid.reshape(pair_count, hemis, field_count, mode_count, padded), (2, 3, 0, 1, 4)
    )
    balanced_spectra = balanced.reshape(slot_count, 2, field_count, mode_count, totals_count)
    return (balanced_spectra, balanced_grid)


def solution(mesh):
    placed = (P(None, "fld", "lat", None, None), P("lat", "fld", None, None), P(), P("fld"))
    return jax.shard_map(
        per_device,
        mesh=mesh,
        in_specs=placed,
        out_specs=(P("lat", None, None, "fld", None), P(None, "fld", "lat", None, None)),
        check_vma=False,
    )
```
